256 devices in a mesh: groups: 2 (over z), seq: 128 (over x, y, core).
Axes of the slice: x: 8, y: 8, z: 2, core: 2. Of those that a mesh axis runs over, the one named last changes fastest.
The devices are a block of a 8x8x16 slice.
Arguments:
- queries: bfloat16 [64, 128, 576], P('groups', 'seq'), parts along dimension 0, may hold values from -8 to 8
- prefix_pool: bfloat16 [8192, 64, 576], P(('groups', 'seq')), parts along dimension 0, may hold values from -6 to 6
- block_table: int32 [8, 1024], P('groups'), parts along dimension 0, may hold values from 0 to 4095, as said below
- prefix_of: int32 [64], P('groups'), parts along dimension 0, may hold values from 0 to 3
- suffix_cache: bfloat16 [64, 16384, 576], P('groups', 'seq'), parts along dimension 0, may hold values from -24 to 24
- suffix_len: int32 [64], P('groups'), parts along dimension 0, may hold values from 2 to 16384
Outputs:
- context: bfloat16 [64, 128, 512], P('groups', 'seq'), parts along dimension 0
The draws below stay inside these ranges and needn't reach their ends.
There are 2 independent parts, one for each index of `groups`. The reference program is written for one: setup_inputs(seed, part) draws one part's arguments, and reference() takes and returns one part's arrays. A program takes and returns all parts, laid end to end along the dimension named above; each array names one. Nothing has to cross between parts.
Inputs may be any that keep to these rules, and one draw needn't show every extreme that they name: `block_table`: each of the 4096 pool blocks is named exactly once in the table, and of each aligned run of 32 pool blocks exactly 8 belong to each prefix.
All inputs are finite; a program needn't handle non-finite values.
Results may differ from the reference program's by a relative error of at most 0.0033.
Values may be sent and summed in bfloat16 or wider, within the bound.
No kernel may reach another device: no remote copies, remote signals or barrier semaphores. Data moves between devices by JAX's collectives and lax.ppermute only.
A program may use at most 128 MiB of HBM per device.

```python
import jax
import jax.numpy as jnp
from jax import lax

LAT = 512
ROPE = 64
HEADS = 128
BLK = 64
PREFIXES = 4
BLK_DEV = 32
REQS = 32
NBLK = 4096
PBLK = 1024
PLEN = 65536
SUF_MAX = 16384


def base_queries(key):
    values = 1.75 * jax.random.normal(jax.random.fold_in(key, 11), (REQS, HEADS, LAT + ROPE), jnp.float32)
    return jnp.clip(values, -8.0, 8.0)


def draw_queries(key, part):
    return base_queries(key).astype(jnp.bfloat16)


def draw_prefix_of(key, part):
    chosen = jax.random.randint(jax.random.fold_in(key, 21), (REQS,), 0, PREFIXES, dtype=jnp.int32)
    step_size = jax.random.randint(jax.random.fold_in(key, 22), (), 1, PREFIXES, dtype=jnp.int32)
    first = (chosen[1] + step_size) % PREFIXES
    return chosen.at[0].set(first).astype(jnp.int32)


def draw_suffix_cache(key, part):
    suffix_rows = jax.random.normal(jax.random.fold_in(key, 12), (REQS, SUF_MAX, LAT + ROPE), jnp.float32)
    return jnp.clip(suffix_rows, -24.0, 24.0).astype(jnp.bfloat16)


def draw_block_table(key, part):
    holders = NBLK // BLK_DEV
    base = jnp.arange(BLK_DEV, dtype=jnp.int32) % PREFIXES
    device_keys = jax.random.split(jax.random.fold_in(key, 13), holders)
    labels = jax.vmap(lambda one: jax.random.permutation(one, base))(device_keys).reshape(NBLK)
    ranks = jax.random.permutation(jax.random.fold_in(key, 15), NBLK).astype(jnp.int32)
    ordered = jnp.argsort(labels * NBLK + ranks)
    return ordered.reshape(PREFIXES, PBLK).astype(jnp.int32)


def set_ends(values, own_key, low, top_value):
    shape = values.shape
    place = [jax.random.randint(jax.random.fold_in(own_key, axis), (), 0, shape[axis]) for axis in range(len(shape))]
    values = values.at[tuple(place)].set(low)
    longest = shape.index(max(shape))
    place[longest] = (place[longest] + 1) % shape[longest]
    return values.at[tuple(place)].set(top_value)


def block_levels(stream_key, shape, shards, least, high):
    gain = 1.0
    for position, shards_of in shards:
        heights = jax.random.uniform(jax.random.fold_in(jax.random.fold_in(stream_key, 6), position), (shards_of,), jnp.float32, least / len(shards), high / len(shards))
        gain = gain * jnp.repeat(jnp.exp(heights), shape[position] // shards_of).reshape((-1,) + (1,) * (len(shape) - 1 - position))
    return gain


def centred(own_key, dims, deviation, bound, pieces=(), kind=jnp.bfloat16):
    gain = block_levels(own_key, dims, pieces, -0.22, 0.18) if pieces else 1.0
    values = jax.random.normal(own_key, dims, jnp.float32) * deviation * gain
    return jnp.minimum(jnp.maximum(values, -bound), bound).astype(kind)


def setup_inputs(seed: int = 0, part: int = 0) -> dict:
    arg_keys = jax.random.split(jax.random.key(seed), 7)
    part_keys = jax.random.split(jax.random.fold_in(arg_keys[6], part), 7)
    return {
        "queries": draw_queries(jax.random.fold_in(jax.random.fold_in(arg_keys[6], part), 71), part),
        "prefix_pool": centred(part_keys[1], (NBLK, BLK, LAT + ROPE), 1.0, 6.0, ((0, 128),)),
        "block_table": draw_block_table(jax.random.fold_in(jax.random.fold_in(arg_keys[6], part), 71), part),
        "prefix_of": draw_prefix_of(jax.random.fold_in(jax.random.fold_in(arg_keys[6], part), 71), part),
        "suffix_cache": draw_suffix_cache(jax.random.fold_in(jax.random.fold_in(arg_keys[6], part), 71), part),
        "suffix_len": set_ends(jax.random.randint(part_keys[5], (REQS,), 2, SUF_MAX + 1), jax.random.fold_in(part_keys[5], 1), 2, SUF_MAX).astype(jnp.int32),
    }


score_scale = 192.0 ** -0.5


def single(packed, prefix_pool, block_table):
    query_rows, chosen, suffix_rows, length = packed
    blocks = block_table[chosen]
    prefix_keys = prefix_pool[blocks].reshape(PLEN, LAT + ROPE)
    prefix_scores = jnp.dot(query_rows, prefix_keys.T, preferred_element_type=jnp.float32) * score_scale
    suffix_scores = jnp.dot(query_rows, suffix_rows.T, preferred_element_type=jnp.float32) * score_scale
    live_slots = jnp.arange(SUF_MAX, dtype=jnp.int32) < length
    suffix_scores = jnp.where(live_slots[None, :], suffix_scores, -jnp.inf)
    highest = jnp.maximum(jnp.max(prefix_scores, axis=1), jnp.max(suffix_scores, axis=1))
    prefix_weights = jnp.exp(prefix_scores - highest[:, None])
    suffix_weights = jnp.exp(suffix_scores - highest[:, None])
    weight_sum = jnp.sum(prefix_weights, axis=1) + jnp.sum(suffix_weights, axis=1)
    weighted = jnp.dot(prefix_weights.astype(jnp.bfloat16), prefix_keys[:, :LAT], preferred_element_type=jnp.float32)
    weighted = weighted + jnp.dot(suffix_weights.astype(jnp.bfloat16), suffix_rows[:, :LAT], preferred_element_type=jnp.float32)
    return (weighted / weight_sum[:, None]).astype(jnp.bfloat16)


def reference(queries, prefix_pool, block_table, prefix_of, suffix_cache, suffix_len):
    return lax.map(lambda packed: single(packed, prefix_pool, block_table), (queries, prefix_of, suffix_cache, suffix_len))
```

```python
import functools
import math

import jax
import jax.numpy as jnp
from jax import lax
from jax.experimental import pallas as pl
from jax.experimental.pallas import tpu as pltpu
from jax.sharding import PartitionSpec as P

LAT = 512
CORES = 2
LOG2_SCALE = math.log2(math.e) * 192.0 ** (-0.5)
VMEM = pl.BlockSpec(memory_space=pltpu.VMEM)
SMEM = pl.BlockSpec(memory_space=pltpu.SMEM)
ANY = pl.BlockSpec(memory_space=pl.ANY)


class Torus:
    def __init__(self, devices):
        self.devices = devices
        self.side = math.isqrt(devices // CORES)

    def at(self, x, y, core):
        return ((x % self.side) * self.side + y % self.side) * CORES + core

    def groups(self, first):
        n = self.side
        along_x = [[[self.at(x, y, c) for x in range(n)] for y in range(n)] for c in range(CORES)]
        along_y = [[[self.at(x, y, c) for y in range(n)] for x in range(n)] for c in range(CORES)]
        return along_x[0] + along_y[1] if first else along_y[0] + along_x[1]

    def shift(self, value, by):
        n, pairs = self.side, []
        for x in range(n):
            for y in range(n):
                pairs.append((self.at(x, y, 0), self.at(x, y + by, 0)))
                pairs.append((self.at(x, y, 1), self.at(x + by, y, 1)))
        return lax.ppermute(value, "seq", pairs)

    def partner(self, value):
        return lax.ppermute(value, "seq", [(i, i ^ 1) for i in range(self.devices)])


def attend_kernel(
    side, core_ref, label_ref, prefix_ref, live_ref, own_pool, other_pool, own_suffix, other_suffix, *refs
):
    blocks = refs[: side + 1]
    outs = refs[side + 1 : 2 * side + 1]
    keys, tails, stat_m, stat_l, heads, members, counts, sems = refs[2 * side + 1 :]
    prefixes = keys.shape[0]
    held, rows, _ = own_pool.shape
    requests = other_suffix.shape[0]
    slots = other_suffix.shape[1]
    core = core_ref[0]

    for p in range(prefixes):
        counts[p] = 0

    def place(source, first):
        def step(b, carry):
            p = label_ref[first + b]
            at = counts[p]
            counts[p] = at + 1
            start = pl.multiple_of(at * rows, rows)
            pltpu.make_async_copy(source.at[b], keys.at[p, pl.ds(start, rows)], sems.at[0]).start()
            return carry

        lax.fori_loop(0, held, step, 0)

    place(own_pool, core * held)
    place(other_pool, (1 - core) * held)
    own = pltpu.make_async_copy(
        own_suffix.at[pl.ds(core * requests, requests)], tails.at[:, pl.ds(0, slots)], sems.at[1]
    )
    other = pltpu.make_async_copy(other_suffix, tails.at[:, pl.ds(slots, slots)], sems.at[2])
    own.start()
    other.start()

    for p in range(prefixes):
        counts[p] = 0

    def sort(r, carry):
        p = prefix_ref[core * requests + r]
        at = counts[p]
        members[p * requests + at] = r
        counts[p] = at + 1
        return carry

    lax.fori_loop(0, requests, sort, 0)
    stat_m[...] = jnp.zeros_like(stat_m)
    stat_l[...] = jnp.ones_like(stat_l)
    half = requests // 2
    pltpu.make_async_copy(keys, keys, sems.at[0]).wait()
    own.wait()
    other.wait()

    def fetch(r, base):
        for k in range(side):
            span = pl.ds(base + k * blocks[0].shape[1], blocks[0].shape[1])
            if k == side // 2:

                @pl.when(r < half)
                def _():
                    heads[span] = blocks[k][r]

                @pl.when(r >= half)
                def _():
                    heads[span] = blocks[side][r - half]
            else:
                heads[span] = blocks[k][r]

    per = blocks[0].shape[1]
    total = side * per
    nt = (((1,), (1,)), ((), ()))

    def pair(p, i):
        count = counts[p]
        both = [members[p * requests + 2 * i], members[p * requests + jnp.minimum(2 * i + 1, count - 1)]]
        for j in range(2):
            fetch(both[j], j * total)
        q = heads[...]
        front = lax.dot_general(q, keys[p], nt, preferred_element_type=jnp.float32)
        ends, tops = [], []
        slot = lax.broadcasted_iota(jnp.int32, (total, 2 * slots), 1)
        for j in range(2):
            s = lax.dot_general(
                q[j * total : (j + 1) * total], tails[both[j]], nt, preferred_element_type=jnp.float32
            )
            mine, theirs = live_ref[both[j]], live_ref[requests + both[j]]
            limit = jnp.where(slot < slots, mine, theirs + slots)
            s = jnp.where(slot < limit, s, -jnp.inf)
            ends.append(s)
            tops.append(jnp.max(s, axis=1, keepdims=True))
        top = jnp.maximum(jnp.max(front, axis=1, keepdims=True), jnp.concatenate(tops, axis=0))
        top = top.astype(jnp.bfloat16).astype(jnp.float32)

        def split(w):
            high = w.astype(jnp.bfloat16)
            low = (w - high.astype(jnp.float32)).astype(jnp.bfloat16)
            return jnp.concatenate([high, low], axis=0)

        w = jnp.exp2((front - top) * LOG2_SCALE)
        sums = jnp.sum(w, axis=1, keepdims=True)
        o = jnp.dot(split(w), keys[p, :, :LAT], preferred_element_type=jnp.float32)
        o = o[: 2 * total] + o[2 * total :]
        for j in range(2):
            r = both[j]
            here = slice(j * total, (j + 1) * total)
            w = jnp.exp2((ends[j] - top[here]) * LOG2_SCALE)
            l = sums[here] + jnp.sum(w, axis=1, keepdims=True)
            t = jnp.dot(split(w), tails[r, :, :LAT], preferred_element_type=jnp.float32)
            res = o[here] + t[:total] + t[total:]
            for k in range(side):
                outs[k][r] = res[k * per : (k + 1) * per].astype(outs[k].dtype)
            lane = lax.broadcasted_iota(jnp.int32, stat_m.shape, 1)
            stat_m[...] = jnp.where(lane == r, top[here], stat_m[...])
            stat_l[...] = jnp.where(lane == r, l, stat_l[...])

    def prefix(p, carry):
        lax.fori_loop(0, (counts[p] + 1) // 2, lambda i, c: (pair(p, i), c)[1], 0)
        return carry

    lax.fori_loop(0, prefixes, prefix, 0)

    for k in range(side):
        here = slice(k * per, (k + 1) * per)
        l = stat_l[here]
        high = l.astype(jnp.bfloat16)
        low = l - high.astype(jnp.float32)
        parts = [stat_m[here], high.astype(jnp.float32), low, jnp.zeros_like(l)]
        outs[k][requests] = jnp.concatenate(parts, axis=1).astype(outs[k].dtype)


def merge_kernel(*refs):
    parts, out = refs[:-1], refs[-1]
    requests = parts[0].shape[0] - 1
    per = parts[0].shape[1]
    stats = [p[requests].astype(jnp.float32) for p in parts]
    lanes = 128
    tops = [s[:, :lanes] for s in stats]
    sums = [s[:, lanes : 2 * lanes] + s[:, 2 * lanes : 3 * lanes] for s in stats]
    top = functools.reduce(jnp.maximum, tops)
    scales = [jnp.exp2((t - top) * LOG2_SCALE) for t in tops]
    l = functools.reduce(jnp.add, [s * f for s, f in zip(sums, scales)])
    lane = lax.broadcasted_iota(jnp.int32, (per, lanes), 1)
    for r in range(requests):
        acc = None
        for part, f in zip(parts, scales):
            term = part[r].astype(jnp.float32) * f[:, r : r + 1]
            acc = term if acc is None else acc + term
        out[:, r, :LAT] = acc
        out[:, r, LAT:] = jnp.where(lane == 0, top[:, r : r + 1], l[:, r : r + 1])


def finish_kernel(parts, out):
    peers = parts.shape[0]
    for h in range(parts.shape[1]):
        tops = [parts[j, h, :, LAT : LAT + 1] for j in range(peers)]
        top = functools.reduce(jnp.maximum, tops)
        acc, l = None, None
        for j in range(peers):
            f = jnp.exp2((tops[j] - top) * LOG2_SCALE)
            a = parts[j, h, :, :LAT] * f
            b = parts[j, h, :, LAT + 1 : LAT + 2] * f
            acc, l = (a, b) if acc is None else (acc + a, l + b)
        out[h] = (acc / l).astype(out.dtype)


def body(torus, queries, prefix_pool, block_table, prefix_of, suffix_cache, suffix_len):
    side = torus.side
    held, rows, channels = prefix_pool.shape
    prefixes = block_table.shape[0]
    reqs, slots, _ = suffix_cache.shape
    half = reqs // CORES
    position = lax.axis_index("seq")
    core = position % CORES

    q = queries.reshape(CORES, half, channels)
    mine, theirs = q[core], q[1 - core]
    pair_q = jnp.stack([mine, torus.partner(theirs)])
    other_pool = torus.partner(prefix_pool)
    other_suffix = torus.partner(lax.dynamic_slice_in_dim(suffix_cache, (1 - core) * half, half, 0))

    first_block = (position - core) * held
    ids = first_block + lax.iota(jnp.int32, CORES * held)
    named = jnp.any(block_table[:, :, None] == ids[None, None, :], axis=1)
    labels = jnp.sum(named.astype(jnp.int32) * lax.iota(jnp.int32, prefixes)[:, None], axis=0)
    lengths = lax.dynamic_slice_in_dim(suffix_len, core * half, half, 0)
    live = jnp.concatenate([lengths - position * slots, lengths - (position ^ 1) * slots])

    spread = jnp.broadcast_to(pair_q[None], (side,) + pair_q.shape)
    line = lax.all_to_all(spread, "seq", 0, 0, axis_index_groups=torus.groups(True))
    per = side * CORES
    block = jnp.swapaxes(line.reshape(per, half, channels), 0, 1)

    got = {0: block}
    mid = half // 2
    for k in (2, side - 2, 1, side - 1):
        got[k] = torus.shift(block, k)
    got[3] = torus.shift(got[2], 1)
    got[side - 3] = torus.shift(got[side - 2], side - 1)
    got[4] = torus.shift(got[2][:mid], 2)
    got[side] = torus.shift(got[side - 2][mid:], side - 2)

    shape = (half + 1, per, LAT)
    outs = pl.pallas_call(
        functools.partial(attend_kernel, side),
        out_shape=[jax.ShapeDtypeStruct(shape, jnp.float32)]
        + [jax.ShapeDtypeStruct(shape, jnp.bfloat16)] * (side - 1),
        in_specs=[SMEM] * 4 + [ANY] * 4 + [VMEM] * (side + 1),
        out_specs=[VMEM] * side,
        scratch_shapes=[
            pltpu.VMEM((prefixes, CORES * held // prefixes * rows, channels), jnp.bfloat16),
            pltpu.VMEM((half, CORES * slots, channels), jnp.bfloat16),
            pltpu.VMEM((side * per, 128), jnp.float32),
            pltpu.VMEM((side * per, 128), jnp.float32),
            pltpu.VMEM((2 * side * per, channels), jnp.bfloat16),
            pltpu.SMEM((prefixes * half,), jnp.int32),
            pltpu.SMEM((prefixes,), jnp.int32),
            pltpu.SemaphoreType.DMA((3,)),
        ],
        name="attend",
    )(
        core.reshape(1),
        labels,
        prefix_of,
        live,
        prefix_pool,
        other_pool,
        suffix_cache,
        other_suffix,
        *[got[k] for k in range(side + 1)],
    )

    parts = [outs[0]] + [torus.shift(outs[k], side - k) for k in (4, 3, 5, 2, 6, 1, 7)]
    merged = pl.pallas_call(
        merge_kernel,
        out_shape=jax.ShapeDtypeStruct((per, half, LAT + 128), jnp.float32),
        in_specs=[VMEM] * side,
        out_specs=VMEM,
        name="merge",
    )(*parts)
    shares = lax.all_to_all(
        merged.reshape(side, CORES, half, LAT + 128), "seq", 0, 0, axis_index_groups=torus.groups(True)
    )
    context = pl.pallas_call(
        finish_kernel,
        out_shape=jax.ShapeDtypeStruct((CORES, half, LAT), jnp.bfloat16),
        in_specs=[VMEM],
        out_specs=VMEM,
        name="finish",
    )(shares)
    back = torus.partner(context[1])
    both = jnp.where(core == 0, jnp.stack([context[0], back]), jnp.stack([back, context[0]]))
    return both.reshape(reqs, 1, LAT)


def solution(mesh):
    torus = Torus(mesh.shape["seq"])
    return jax.shard_map(
        functools.partial(body, torus),
        mesh=mesh,
        in_specs=(
            P("groups", "seq", None),
            P(("groups", "seq"), None, None),
            P("groups", None),
            P("groups"),
            P("groups", "seq", None),
            P("groups"),
        ),
        out_specs=P("groups", "seq", None),
        check_vma=False,
    )
```

```python
import functools
import math

import jax
import jax.numpy as jnp
from jax import lax
from jax.experimental import pallas as pl
from jax.experimental.pallas import tpu as pltpu
from jax.sharding import PartitionSpec as P


LAT = 512
PARTS = 2
WIDE = 2
CORES = 2
LOG2_SCALE = math.log2(math.e) * 192.0 ** (-0.5)
VMEM = pl.BlockSpec(memory_space=pltpu.VMEM)
SMEM = pl.BlockSpec(memory_space=pltpu.SMEM)
ANY = pl.BlockSpec(memory_space=pl.ANY)


class Torus:
    def __init__(self, devices):
        self.devices = devices
        self.side = math.isqrt(devices // CORES)

    def at(self, x, y, core):
        return ((x % self.side) * self.side + y % self.side) * CORES + core

    def groups(self, first):
        n = self.side
        along_x = [[[self.at(x, y, c) for x in range(n)] for y in range(n)] for c in range(CORES)]
        along_y = [[[self.at(x, y, c) for y in range(n)] for x in range(n)] for c in range(CORES)]
        return along_x[0] + along_y[1] if first else along_y[0] + along_x[1]

    def shift(self, value, by):
        n, pairs = self.side, []
        for x in range(n):
            for y in range(n):
                pairs.append((self.at(x, y, 0), self.at(x, y + by, 0)))
                pairs.append((self.at(x, y, 1), self.at(x + by, y, 1)))
        return lax.ppermute(value, "seq", pairs)

    def partner(self, value):
        return lax.ppermute(value, "seq", [(i, i ^ 1) for i in range(self.devices)])


def stage_kernel(core_ref, label_ref, own_pool, other_pool, out, keys, counts, sems):
    prefixes = keys.shape[0]
    held, rows, _ = own_pool.shape
    core = core_ref[0]
    for p in range(prefixes):
        counts[p] = 0

    def place(source, first):
        def step(b, carry):
            p = label_ref[first + b]
            at = counts[p]
            counts[p] = at + 1
            start = pl.multiple_of(at * rows, rows)
            pltpu.make_async_copy(source.at[b], keys.at[p, pl.ds(start, rows)], sems.at[p]).start()
            return carry

        lax.fori_loop(0, held, step, 0)

    place(own_pool, core * held)
    place(other_pool, (1 - core) * held)
    copies = []
    for p in range(prefixes):
        pltpu.make_async_copy(keys.at[p], keys.at[p], sems.at[p]).wait()
        copies.append(pltpu.make_async_copy(keys.at[p], out.at[p], sems.at[prefixes + p]))
        copies[p].start()
    for copy in copies:
        copy.wait()


def attend_kernel(core_ref, prefix_ref, live_ref, sorted_keys, own_suffix, other_suffix, *refs):
    *refs, keys, tails, stat_m, stat_l, heads, members, counts, key_sems, tail_sems = refs
    n = len(refs) // 2
    halved = n // 2
    half = prefix_ref.shape[0] // CORES // 2
    blocks, outs = refs[: len(refs) - n], refs[len(refs) - n :]
    prefixes = keys.shape[0]
    requests, _, spots = tails.shape
    slots = spots // CORES
    per = outs[0].shape[1]
    total = n * per
    core = core_ref[0]

    for p in range(prefixes):
        counts[p] = 0

    def sort(r, carry):
        p = prefix_ref[core * requests + r]
        at = counts[p]
        members[p * requests + at] = r
        counts[p] = at + 1
        return carry

    lax.fori_loop(0, requests, sort, 0)

    def key_copy(p):
        return pltpu.make_async_copy(sorted_keys.at[p], keys.at[p], key_sems.at[p])

    def load(p, carry):
        key_copy(p).start()

        def tail(i, carry):
            r = members[p * requests + i]
            mine, theirs = tails.at[r, :, pl.ds(0, slots)], tails.at[r, :, pl.ds(slots, slots)]
            pltpu.make_async_copy(own_suffix.at[core * requests + r], mine, tail_sems.at[r]).start()
            pltpu.make_async_copy(other_suffix.at[core * requests + r], theirs, tail_sems.at[r]).start()
            return carry

        lax.fori_loop(0, counts[p], tail, 0)
        return carry

    lax.fori_loop(0, prefixes, load, 0)
    stat_m[...] = jnp.zeros_like(stat_m)
    stat_l[...] = jnp.ones_like(stat_l)
    nt = (((1,), (1,)), ((), ()))

    def fetch(r, base):
        for k in range(n):
            span = pl.ds(base + k * per, per)
            if k != halved:
                heads[span] = blocks[k][r]
                continue

            @pl.when(r < half)
            def _():
                heads[span] = blocks[k][r]

            @pl.when(r >= half)
            def _():
                heads[span] = blocks[n][r - half]

    def split(w):
        high = w.astype(jnp.bfloat16)
        low = (w - high.astype(jnp.float32)).astype(jnp.bfloat16)
        return jnp.concatenate([high, low], axis=0)

    def group(p, i):
        last = counts[p] - 1
        rs = [members[p * requests + jnp.minimum(WIDE * i + j, last)] for j in range(WIDE)]
        for j in range(WIDE):
            fetch(rs[j], j * total)

            @pl.when(WIDE * i + j <= last)
            def _():
                pltpu.make_async_copy(tails.at[rs[j]], tails.at[rs[j]], tail_sems.at[rs[j]]).wait()

        q = heads[...]
        cuts = keys.shape[1] // PARTS
        fronts, tops = [], []
        for c in range(PARTS):
            part = keys[p, c * cuts : (c + 1) * cuts]
            f = lax.dot_general(q, part, nt, preferred_element_type=jnp.float32)
            fronts.append(f)
            tops.append(jnp.max(f, axis=1, keepdims=True))
        slot = lax.broadcasted_iota(jnp.int32, (total, spots), 1)
        o, sums = None, None
        best = functools.reduce(jnp.maximum, tops)
        ends, edge = [], []
        for j in range(WIDE):
            s = jnp.dot(q[j * total : (j + 1) * total], tails[rs[j]], preferred_element_type=jnp.float32)
            mine, theirs = live_ref[rs[j]], live_ref[requests + rs[j]]
            limit = jnp.where(slot < slots, mine, theirs + slots)
            s = jnp.where(slot < limit, s, -jnp.inf)
            ends.append(s)
            edge.append(jnp.max(s, axis=1, keepdims=True))
        top = jnp.maximum(best, jnp.concatenate(edge, axis=0)).astype(jnp.bfloat16).astype(jnp.float32)
        for c in range(PARTS):
            w = jnp.exp2((fronts[c] - tops[c]) * LOG2_SCALE)
            fix = jnp.exp2((tops[c] - top) * LOG2_SCALE)
            t = jnp.dot(split(w), keys[p, c * cuts : (c + 1) * cuts, :LAT], preferred_element_type=jnp.float32)
            t = (t[: WIDE * total] + t[WIDE * total :]) * fix
            l = jnp.sum(w, axis=1, keepdims=True) * fix
            o, sums = (t, l) if o is None else (o + t, sums + l)
        for j in range(WIDE):
            r = rs[j]
            here = slice(j * total, (j + 1) * total)
            w = jnp.exp2((ends[j] - top[here]) * LOG2_SCALE)
            l = sums[here] + jnp.sum(w, axis=1, keepdims=True)
            t = lax.dot_general(split(w), tails[r, :LAT], nt, preferred_element_type=jnp.float32)
            res = o[here] + t[:total] + t[total:]
            for k in range(n):
                outs[k][r] = res[k * per : (k + 1) * per].astype(outs[k].dtype)
            lane = lax.broadcasted_iota(jnp.int32, stat_m.shape, 1)
            stat_m[...] = jnp.where(lane == r, top[here], stat_m[...])
            stat_l[...] = jnp.where(lane == r, l, stat_l[...])

    def prefix(p, carry):
        key_copy(p).wait()
        lax.fori_loop(0, (counts[p] + WIDE - 1) // WIDE, lambda i, c: (group(p, i), c)[1], 0)
        return carry

    lax.fori_loop(0, prefixes, prefix, 0)

    for k in range(n):
        here = slice(k * per, (k + 1) * per)
        l = stat_l[here]
        high = l.astype(jnp.bfloat16).astype(jnp.float32)
        parts = [stat_m[here], high, l - high, jnp.zeros_like(l)]
        outs[k][requests] = jnp.concatenate(parts, axis=1).astype(outs[k].dtype)


def merge_kernel(*refs):
    parts, out = refs[:-1], refs[-1]
    requests = parts[0].shape[0] - 1
    per = parts[0].shape[1]
    stats = [p[requests].astype(jnp.float32) for p in parts]
    lanes = 128
    tops = [s[:, :lanes] for s in stats]
    sums = [s[:, lanes : 2 * lanes] + s[:, 2 * lanes : 3 * lanes] for s in stats]
    top = functools.reduce(jnp.maximum, tops)
    scales = [jnp.exp2((t - top) * LOG2_SCALE) for t in tops]
    l = functools.reduce(jnp.add, [s * f for s, f in zip(sums, scales)])
    lane = lax.broadcasted_iota(jnp.int32, (per, lanes), 1)
    for r in range(requests):
        acc = None
        for part, f in zip(parts, scales):
            term = part[r].astype(jnp.float32) * f[:, r : r + 1]
            acc = term if acc is None else acc + term
        out[:, r, :LAT] = acc
        out[:, r, LAT:] = jnp.where(lane == 0, top[:, r : r + 1], l[:, r : r + 1])


def finish_kernel(parts, out):
    peers = parts.shape[0]
    for h in range(parts.shape[1]):
        tops = [parts[j, h, :, LAT : LAT + 1] for j in range(peers)]
        top = functools.reduce(jnp.maximum, tops)
        acc, l = None, None
        for j in range(peers):
            f = jnp.exp2((tops[j] - top) * LOG2_SCALE)
            a = parts[j, h, :, :LAT] * f
            b = parts[j, h, :, LAT + 1 : LAT + 2] * f
            acc, l = (a, b) if acc is None else (acc + a, l + b)
        out[h] = (acc / l).astype(out.dtype)


def stage(core, labels, own_pool, other_pool, prefixes):
    held, rows, channels = own_pool.shape
    keys = (prefixes, CORES * held // prefixes * rows, channels)
    own_pool = pltpu.with_memory_space_constraint(own_pool, pltpu.HBM)
    return pl.pallas_call(
        stage_kernel,
        out_shape=pltpu.HBM(keys, jnp.bfloat16),
        in_specs=[SMEM] * 2 + [ANY] * 2,
        out_specs=ANY,
        scratch_shapes=[
            pltpu.VMEM(keys, jnp.bfloat16),
            pltpu.SMEM((prefixes,), jnp.int32),
            pltpu.SemaphoreType.DMA((2 * prefixes,)),
        ],
        compiler_params=pltpu.CompilerParams(vmem_limit_bytes=8 * 2**20),
        cost_estimate=pl.CostEstimate(flops=4 * 10**9, bytes_accessed=0, transcendentals=0),
        name="stage",
    )(core, labels, own_pool, other_pool)


def attend(core, prefix_of, live, keys, own_suffix, other_suffix, blocks, dtypes):
    n = len(dtypes)
    half, per, channels = blocks[0].shape
    prefixes = keys.shape[0]
    tails = (half, channels, CORES * other_suffix.shape[2])
    flops = 6 * half * n * per * channels * (keys.shape[1] + tails[2])
    keys, own_suffix, other_suffix = (
        pltpu.with_memory_space_constraint(a, pltpu.HBM) for a in (keys, own_suffix, other_suffix)
    )
    return pl.pallas_call(
        attend_kernel,
        out_shape=[jax.ShapeDtypeStruct((half + 1, per, LAT), t) for t in dtypes],
        in_specs=[SMEM] * 3 + [ANY] * 3 + [VMEM] * len(blocks),
        out_specs=[VMEM] * n,
        scratch_shapes=[
            pltpu.VMEM(keys.shape, jnp.bfloat16),
            pltpu.VMEM(tails, jnp.bfloat16),
            pltpu.VMEM((n * per, 128), jnp.float32),
            pltpu.VMEM((n * per, 128), jnp.float32),
            pltpu.VMEM((WIDE * n * per, channels), jnp.bfloat16),
            pltpu.SMEM((prefixes * half,), jnp.int32),
            pltpu.SMEM((prefixes,), jnp.int32),
            pltpu.SemaphoreType.DMA((prefixes,)),
            pltpu.SemaphoreType.DMA((half,)),
        ],
        compiler_params=pltpu.CompilerParams(vmem_limit_bytes=36 * 2**20),
        cost_estimate=pl.CostEstimate(flops=flops, bytes_accessed=0, transcendentals=0),
        name="attend",
    )(core, prefix_of, live, keys, own_suffix, other_suffix, *blocks)


def body(torus, queries, prefix_pool, block_table, prefix_of, suffix_cache, suffix_len):
    side = torus.side
    held, _, channels = prefix_pool.shape
    prefixes = block_table.shape[0]
    reqs, slots, _ = suffix_cache.shape
    half = reqs // CORES
    position = lax.axis_index("seq")
    core = position % CORES

    q = queries.reshape(CORES, half, channels)
    mine, theirs = q[core], q[1 - core]
    theirs = torus.partner(theirs)
    suffix = jnp.swapaxes(suffix_cache, 1, 2)
    pool, theirs = lax.optimization_barrier((prefix_pool, theirs))
    pair_q = jnp.stack([mine, theirs])
    other_pool = torus.partner(pool)
    other_suffix = torus.partner(suffix)

    first_block = (position - core) * held
    ids = first_block + lax.iota(jnp.int32, CORES * held)
    named = jnp.any(block_table[:, :, None] == ids[None, None, :], axis=1)
    labels = jnp.sum(named.astype(jnp.int32) * lax.iota(jnp.int32, prefixes)[:, None], axis=0)
    lengths = lax.dynamic_slice_in_dim(suffix_len, core * half, half, 0)
    live = jnp.concatenate([lengths - position * slots, lengths - (position ^ 1) * slots])

    spread = jnp.broadcast_to(pair_q[None], (side,) + pair_q.shape)
    line = lax.all_to_all(spread, "seq", 0, 0, axis_index_groups=torus.groups(True))
    per = side * CORES
    block = jnp.swapaxes(line.reshape(per, half, channels), 0, 1)

    order = (4, 3, side - 3, 2, side - 2, 1, side - 1)
    got = {0: block}
    mid = half // 2
    for k in (2, side - 2, 1, side - 1):
        got[k] = torus.shift(block, k)
    got[4] = torus.shift(got[2][:mid], 2)
    got[side] = torus.shift(got[side - 2][mid:], side - 2)
    got[3] = torus.shift(got[2], 1)
    got[side - 3] = torus.shift(got[side - 2], side - 1)

    core = core.reshape(1)
    keys = stage(core, labels, prefix_pool, other_pool, prefixes)
    types = [jnp.float32] + [jnp.bfloat16] * (side - 1)
    outs = attend(core, prefix_of, live, keys, suffix, other_suffix, [got[k] for k in range(side + 1)], types)
    parts = [outs[0]] + [torus.shift(outs[k], side - k) for k in order]
    merged = pl.pallas_call(
        merge_kernel,
        out_shape=jax.ShapeDtypeStruct((per, half, LAT + 128), jnp.float32),
        in_specs=[VMEM] * side,
        out_specs=VMEM,
        compiler_params=pltpu.CompilerParams(vmem_limit_bytes=16 * 2**20),
        name="merge",
    )(*parts)
    shares = lax.all_to_all(
        merged.reshape(side, CORES, half, LAT + 128), "seq", 0, 0, axis_index_groups=torus.groups(True)
    )
    context = pl.pallas_call(
        finish_kernel,
        out_shape=jax.ShapeDtypeStruct((CORES, half, LAT), jnp.bfloat16),
        in_specs=[VMEM],
        out_specs=VMEM,
        compiler_params=pltpu.CompilerParams(vmem_limit_bytes=8 * 2**20),
        name="finish",
    )(shares)
    back = torus.partner(context[1])
    both = jnp.where(core[0] == 0, jnp.stack([context[0], back]), jnp.stack([back, context[0]]))
    return both.reshape(reqs, 1, LAT)


def solution(mesh):
    torus = Torus(mesh.shape["seq"])

    def step(*args):
        return body(torus, *args)

    return jax.shard_map(
        step,
        mesh=mesh,
        in_specs=(
            P("groups", "seq", None),
            P(("groups", "seq"), None, None),
            P("groups", None),
            P("groups"),
            P("groups", "seq", None),
            P("groups"),
        ),
        out_specs=P("groups", "seq", None),
        check_vma=False,
    )
```

```python
import functools
import math

import jax
import jax.numpy as jnp
from jax import lax
from jax.experimental import pallas as pl
from jax.experimental.pallas import tpu as pltpu
from jax.sharding import PartitionSpec as P


LAT = 512
PARTS = 2
WIDE = 2
CORES = 2
LOG2_SCALE = math.log2(math.e) * 192.0 ** (-0.5)
VMEM = pl.BlockSpec(memory_space=pltpu.VMEM)
SMEM = pl.BlockSpec(memory_space=pltpu.SMEM)
ANY = pl.BlockSpec(memory_space=pl.ANY)


class Torus:
    def __init__(self, devices):
        self.devices = devices
        self.side = math.isqrt(devices // CORES)

    def at(self, x, y, core):
        return ((x % self.side) * self.side + y % self.side) * CORES + core

    def groups(self, first):
        n = self.side
        along_x = [[[self.at(x, y, c) for x in range(n)] for y in range(n)] for c in range(CORES)]
        along_y = [[[self.at(x, y, c) for y in range(n)] for x in range(n)] for c in range(CORES)]
        return along_y[0] + along_x[1] if first else along_x[0] + along_y[1]

    def shift(self, value, by):
        n, pairs = self.side, []
        for x in range(n):
            for y in range(n):
                pairs.append((self.at(x, y, 0), self.at(x + by, y, 0)))
                pairs.append((self.at(x, y, 1), self.at(x, y + by, 1)))
        return lax.ppermute(value, "seq", pairs)

    def partner(self, value):
        return lax.ppermute(value, "seq", [(i, i ^ 1) for i in range(self.devices)])


def stage_kernel(core_ref, label_ref, own_pool, other_pool, out, keys, counts, sems):
    prefixes = keys.shape[0]
    held, rows, _ = own_pool.shape
    core = core_ref[0]
    for p in range(prefixes):
        counts[p] = 0

    def place(source, first):
        def step(b, carry):
            p = label_ref[first + b]
            at = counts[p]
            counts[p] = at + 1
            start = pl.multiple_of(at * rows, rows)
            pltpu.make_async_copy(source.at[b], keys.at[p, pl.ds(start, rows)], sems.at[p]).start()
            return carry

        lax.fori_loop(0, held, step, 0)

    place(own_pool, core * held)
    place(other_pool, (1 - core) * held)
    copies = []
    for p in range(prefixes):
        pltpu.make_async_copy(keys.at[p], keys.at[p], sems.at[p]).wait()
        copies.append(pltpu.make_async_copy(keys.at[p], out.at[p], sems.at[prefixes + p]))
        copies[p].start()
    for copy in copies:
        copy.wait()


def attend_kernel(core_ref, prefix_ref, live_ref, sorted_keys, own_suffix, other_suffix, *refs):
    *refs, keys, tails, stat_m, stat_l, heads, members, counts, key_sems, tail_sems = refs
    n = len(refs) // 2
    halved = n // 2
    half = prefix_ref.shape[0] // CORES // 2
    blocks, outs = refs[: len(refs) - n], refs[len(refs) - n :]
    prefixes = keys.shape[0]
    requests, _, spots = tails.shape
    slots = spots // CORES
    per = outs[0].shape[1]
    total = n * per
    core = core_ref[0]

    for p in range(prefixes):
        counts[p] = 0

    def sort(r, carry):
        p = prefix_ref[core * requests + r]
        at = counts[p]
        members[p * requests + at] = r
        counts[p] = at + 1
        return carry

    lax.fori_loop(0, requests, sort, 0)

    def key_copy(p):
        return pltpu.make_async_copy(sorted_keys.at[p], keys.at[p], key_sems.at[p])

    def load(p, carry):
        key_copy(p).start()

        def tail(i, carry):
            r = members[p * requests + i]
            mine, theirs = tails.at[r, :, pl.ds(0, slots)], tails.at[r, :, pl.ds(slots, slots)]
            pltpu.make_async_copy(own_suffix.at[core * requests + r], mine, tail_sems.at[r]).start()
            pltpu.make_async_copy(other_suffix.at[core * requests + r], theirs, tail_sems.at[r]).start()
            return carry

        lax.fori_loop(0, counts[p], tail, 0)
        return carry

    lax.fori_loop(0, prefixes, load, 0)
    stat_m[...] = jnp.zeros_like(stat_m)
    stat_l[...] = jnp.ones_like(stat_l)
    nt = (((1,), (1,)), ((), ()))

    def fetch(r, base):
        for k in range(n):
            span = pl.ds(base + k * per, per)
            if k != halved:
                heads[span] = blocks[k][r]
                continue

            @pl.when(r < half)
            def _():
                heads[span] = blocks[k][r]

            @pl.when(r >= half)
            def _():
                heads[span] = blocks[n][r - half]

    def split(w):
        high = w.astype(jnp.bfloat16)
        low = (w - high.astype(jnp.float32)).astype(jnp.bfloat16)
        return jnp.concatenate([high, low], axis=0)

    def group(p, i):
        last = counts[p] - 1
        rs = [members[p * requests + jnp.minimum(WIDE * i + j, last)] for j in range(WIDE)]
        for j in range(WIDE):
            fetch(rs[j], j * total)

            @pl.when(WIDE * i + j <= last)
            def _():
                pltpu.make_async_copy(tails.at[rs[j]], tails.at[rs[j]], tail_sems.at[rs[j]]).wait()

        q = heads[...]
        cuts = keys.shape[1] // PARTS
        fronts, tops = [], []
        for c in range(PARTS):
            part = keys[p, c * cuts : (c + 1) * cuts]
            f = lax.dot_general(q, part, nt, preferred_element_type=jnp.float32)
            fronts.append(f)
            tops.append(jnp.max(f, axis=1, keepdims=True))
        slot = lax.broadcasted_iota(jnp.int32, (total, spots), 1)
        o, sums = None, None
        best = functools.reduce(jnp.maximum, tops)
        ends, edge = [], []
        for j in range(WIDE):
            s = jnp.dot(q[j * total : (j + 1) * total], tails[rs[j]], preferred_element_type=jnp.float32)
            mine, theirs = live_ref[rs[j]], live_ref[requests + rs[j]]
            limit = jnp.where(slot < slots, mine, theirs + slots)
            s = jnp.where(slot < limit, s, -jnp.inf)
            ends.append(s)
            edge.append(jnp.max(s, axis=1, keepdims=True))
        top = jnp.maximum(best, jnp.concatenate(edge, axis=0)).astype(jnp.bfloat16).astype(jnp.float32)
        for c in range(PARTS):
            w = jnp.exp2((fronts[c] - tops[c]) * LOG2_SCALE)
            fix = jnp.exp2((tops[c] - top) * LOG2_SCALE)
            t = jnp.dot(split(w), keys[p, c * cuts : (c + 1) * cuts, :LAT], preferred_element_type=jnp.float32)
            t = (t[: WIDE * total] + t[WIDE * total :]) * fix
            l = jnp.sum(w, axis=1, keepdims=True) * fix
            o, sums = (t, l) if o is None else (o + t, sums + l)
        for j in range(WIDE):
            r = rs[j]
            here = slice(j * total, (j + 1) * total)
            w = jnp.exp2((ends[j] - top[here]) * LOG2_SCALE)
            l = sums[here] + jnp.sum(w, axis=1, keepdims=True)
            t = lax.dot_general(split(w), tails[r, :LAT], nt, preferred_element_type=jnp.float32)
            res = o[here] + t[:total] + t[total:]
            for k in range(n):
                outs[k][r] = res[k * per : (k + 1) * per].astype(outs[k].dtype)
            lane = lax.broadcasted_iota(jnp.int32, stat_m.shape, 1)
            stat_m[...] = jnp.where(lane == r, top[here], stat_m[...])
            stat_l[...] = jnp.where(lane == r, l, stat_l[...])

    def prefix(p, carry):
        key_copy(p).wait()
        lax.fori_loop(0, (counts[p] + WIDE - 1) // WIDE, lambda i, c: (group(p, i), c)[1], 0)
        return carry

    lax.fori_loop(0, prefixes, prefix, 0)

    for k in range(n):
        here = slice(k * per, (k + 1) * per)
        l = stat_l[here]
        high = l.astype(jnp.bfloat16).astype(jnp.float32)
        parts = [stat_m[here], high, l - high, jnp.zeros_like(l)]
        outs[k][requests] = jnp.concatenate(parts, axis=1).astype(outs[k].dtype)


def merge_kernel(*refs):
    parts, out = refs[:-1], refs[-1]
    requests = parts[0].shape[0] - 1
    per = parts[0].shape[1]
    stats = [p[requests].astype(jnp.float32) for p in parts]
    lanes = 128
    tops = [s[:, :lanes] for s in stats]
    sums = [s[:, lanes : 2 * lanes] + s[:, 2 * lanes : 3 * lanes] for s in stats]
    top = functools.reduce(jnp.maximum, tops)
    scales = [jnp.exp2((t - top) * LOG2_SCALE) for t in tops]
    l = functools.reduce(jnp.add, [s * f for s, f in zip(sums, scales)])
    lane = lax.broadcasted_iota(jnp.int32, (per, lanes), 1)
    for r in range(requests):
        acc = None
        for part, f in zip(parts, scales):
            term = part[r].astype(jnp.float32) * f[:, r : r + 1]
            acc = term if acc is None else acc + term
        out[:, r, :LAT] = acc
        out[:, r, LAT:] = jnp.where(lane == 0, top[:, r : r + 1], l[:, r : r + 1])


def finish_kernel(parts, out):
    peers = parts.shape[0]
    for h in range(parts.shape[1]):
        tops = [parts[j, h, :, LAT : LAT + 1] for j in range(peers)]
        top = functools.reduce(jnp.maximum, tops)
        acc, l = None, None
        for j in range(peers):
            f = jnp.exp2((tops[j] - top) * LOG2_SCALE)
            a = parts[j, h, :, :LAT] * f
            b = parts[j, h, :, LAT + 1 : LAT + 2] * f
            acc, l = (a, b) if acc is None else (acc + a, l + b)
        out[h] = (acc / l).astype(out.dtype)


def stage(core, labels, own_pool, other_pool, prefixes):
    held, rows, channels = own_pool.shape
    keys = (prefixes, CORES * held // prefixes * rows, channels)
    own_pool = pltpu.with_memory_space_constraint(own_pool, pltpu.HBM)
    return pl.pallas_call(
        stage_kernel,
        out_shape=pltpu.HBM(keys, jnp.bfloat16),
        in_specs=[SMEM] * 2 + [ANY] * 2,
        out_specs=ANY,
        scratch_shapes=[
            pltpu.VMEM(keys, jnp.bfloat16),
            pltpu.SMEM((prefixes,), jnp.int32),
            pltpu.SemaphoreType.DMA((2 * prefixes,)),
        ],
        compiler_params=pltpu.CompilerParams(vmem_limit_bytes=8 * 2**20),
        cost_estimate=pl.CostEstimate(flops=4 * 10**9, bytes_accessed=0, transcendentals=0),
        name="stage",
    )(core, labels, own_pool, other_pool)


def attend(core, prefix_of, live, keys, own_suffix, other_suffix, blocks, dtypes):
    n = len(dtypes)
    half, per, channels = blocks[0].shape
    prefixes = keys.shape[0]
    tails = (half, channels, CORES * other_suffix.shape[2])
    flops = 6 * half * n * per * channels * (keys.shape[1] + tails[2])
    keys, own_suffix, other_suffix = (
        pltpu.with_memory_space_constraint(a, pltpu.HBM) for a in (keys, own_suffix, other_suffix)
    )
    return pl.pallas_call(
        attend_kernel,
        out_shape=[jax.ShapeDtypeStruct((half + 1, per, LAT), t) for t in dtypes],
        in_specs=[SMEM] * 3 + [ANY] * 3 + [VMEM] * len(blocks),
        out_specs=[VMEM] * n,
        scratch_shapes=[
            pltpu.VMEM(keys.shape, jnp.bfloat16),
            pltpu.VMEM(tails, jnp.bfloat16),
            pltpu.VMEM((n * per, 128), jnp.float32),
            pltpu.VMEM((n * per, 128), jnp.float32),
            pltpu.VMEM((WIDE * n * per, channels), jnp.bfloat16),
            pltpu.SMEM((prefixes * half,), jnp.int32),
            pltpu.SMEM((prefixes,), jnp.int32),
            pltpu.SemaphoreType.DMA((prefixes,)),
            pltpu.SemaphoreType.DMA((half,)),
        ],
        compiler_params=pltpu.CompilerParams(vmem_limit_bytes=36 * 2**20),
        cost_estimate=pl.CostEstimate(flops=flops, bytes_accessed=0, transcendentals=0),
        name="attend",
    )(core, prefix_of, live, keys, own_suffix, other_suffix, *blocks)


def body(torus, queries, prefix_pool, block_table, prefix_of, suffix_cache, suffix_len):
    side = torus.side
    held, _, channels = prefix_pool.shape
    prefixes = block_table.shape[0]
    reqs, slots, _ = suffix_cache.shape
    half = reqs // CORES
    position = lax.axis_index("seq")
    core = position % CORES

    q = queries.reshape(CORES, half, channels)
    mine, theirs = q[core], q[1 - core]
    theirs = torus.partner(theirs)
    suffix = jnp.swapaxes(suffix_cache, 1, 2)
    pool, theirs = lax.optimization_barrier((prefix_pool, theirs))
    pair_q = jnp.stack([mine, theirs])
    other_pool = torus.partner(pool)
    other_suffix = torus.partner(suffix)

    first_block = (position - core) * held
    ids = first_block + lax.iota(jnp.int32, CORES * held)
    named = jnp.any(block_table[:, :, None] == ids[None, None, :], axis=1)
    labels = jnp.sum(named.astype(jnp.int32) * lax.iota(jnp.int32, prefixes)[:, None], axis=0)
    lengths = lax.dynamic_slice_in_dim(suffix_len, core * half, half, 0)
    live = jnp.concatenate([lengths - position * slots, lengths - (position ^ 1) * slots])

    spread = jnp.broadcast_to(pair_q[None], (side,) + pair_q.shape)
    line = lax.all_to_all(spread, "seq", 0, 0, axis_index_groups=torus.groups(True))
    per = side * CORES
    block = jnp.swapaxes(line.reshape(per, half, channels), 0, 1)

    order = (4, 3, side - 3, 2, side - 2, 1, side - 1)
    got = {0: block}
    mid = half // 2
    for k in (2, side - 2, 1, side - 1):
        got[k] = torus.shift(block, k)
    got[4] = torus.shift(got[2][:mid], 2)
    got[side] = torus.shift(got[side - 2][mid:], side - 2)
    got[3] = torus.shift(got[2], 1)
    got[side - 3] = torus.shift(got[side - 2], side - 1)

    core = core.reshape(1)
    keys = stage(core, labels, prefix_pool, other_pool, prefixes)
    types = [jnp.float32] + [jnp.bfloat16] * (side - 1)
    outs = attend(core, prefix_of, live, keys, suffix, other_suffix, [got[k] for k in range(side + 1)], types)
    parts = [outs[0]] + [torus.shift(outs[k], side - k) for k in order]
    merged = pl.pallas_call(
        merge_kernel,
        out_shape=jax.ShapeDtypeStruct((per, half, LAT + 128), jnp.float32),
        in_specs=[VMEM] * side,
        out_specs=VMEM,
        compiler_params=pltpu.CompilerParams(vmem_limit_bytes=16 * 2**20),
        name="merge",
    )(*parts)
    shares = lax.all_to_all(
        merged.reshape(side, CORES, half, LAT + 128), "seq", 0, 0, axis_index_groups=torus.groups(True)
    )
    context = pl.pallas_call(
        finish_kernel,
        out_shape=jax.ShapeDtypeStruct((CORES, half, LAT), jnp.bfloat16),
        in_specs=[VMEM],
        out_specs=VMEM,
        compiler_params=pltpu.CompilerParams(vmem_limit_bytes=8 * 2**20),
        name="finish",
    )(shares)
    back = torus.partner(context[1])
    both = jnp.where(core[0] == 0, jnp.stack([context[0], back]), jnp.stack([back, context[0]]))
    return both.reshape(reqs, 1, LAT)


def solution(mesh):
    torus = Torus(mesh.shape["seq"])

    def step(*args):
        return body(torus, *args)

    return jax.shard_map(
        step,
        mesh=mesh,
        in_specs=(
            P("groups", "seq", None),
            P(("groups", "seq"), None, None),
            P("groups", None),
            P("groups"),
            P("groups", "seq", None),
            P("groups"),
        ),
        out_specs=P("groups", "seq", None),
        check_vma=False,
    )
```

```python
import functools
import math

import jax
import jax.numpy as jnp
from jax import lax
from jax.experimental import pallas as pl
from jax.experimental.pallas import tpu as pltpu
from jax.sharding import PartitionSpec as P


LAT = 512
LANES = 128
PARTS = 2
WIDE = 2
CORES = 2
LOG2_SCALE = math.log2(math.e) * 192.0 ** (-0.5)
VMEM = pl.BlockSpec(memory_space=pltpu.VMEM)
SMEM = pl.BlockSpec(memory_space=pltpu.SMEM)
ANY = pl.BlockSpec(memory_space=pl.ANY)


class Torus:
    def __init__(self, devices):
        self.devices = devices
        self.side = math.isqrt(devices // CORES)

    def at(self, x, y, core):
        return ((x % self.side) * self.side + y % self.side) * CORES + core

    def groups(self, first):
        n = self.side
        along_x = [[[self.at(x, y, c) for x in range(n)] for y in range(n)] for c in range(CORES)]
        along_y = [[[self.at(x, y, c) for y in range(n)] for x in range(n)] for c in range(CORES)]
        return along_y[0] + along_x[1] if first else along_x[0] + along_y[1]

    def shift(self, value, by):
        n, pairs = self.side, []
        for x in range(n):
            for y in range(n):
                pairs.append((self.at(x, y, 0), self.at(x + by, y, 0)))
                pairs.append((self.at(x, y, 1), self.at(x, y + by, 1)))
        return lax.ppermute(value, "seq", pairs)

    def partner(self, value):
        return lax.ppermute(value, "seq", [(i, i ^ 1) for i in range(self.devices)])


def stage_kernel(core_ref, label_ref, own_pool, other_pool, out, keys, counts, sems):
    prefixes = keys.shape[0]
    held, rows, _ = own_pool.shape
    core = core_ref[0]
    for p in range(prefixes):
        counts[p] = 0

    def place(source, first):
        def step(b, carry):
            p = label_ref[first + b]
            at = counts[p]
            counts[p] = at + 1
            start = pl.multiple_of(at * rows, rows)
            pltpu.make_async_copy(source.at[b], keys.at[p, pl.ds(start, rows)], sems.at[p]).start()
            return carry

        lax.fori_loop(0, held, step, 0)

    place(own_pool, core * held)
    place(other_pool, (1 - core) * held)
    copies = []
    for p in range(prefixes):
        pltpu.make_async_copy(keys.at[p], keys.at[p], sems.at[p]).wait()
        copies.append(pltpu.make_async_copy(keys.at[p], out.at[p], sems.at[prefixes + p]))
        copies[p].start()
    for copy in copies:
        copy.wait()


def attend_kernel(core_ref, prefix_ref, live_ref, sorted_keys, own_suffix, other_suffix, *refs):
    *refs, keys, tails, stats, heads, members, counts, key_sems, tail_sems = refs
    n = len(refs) // 2
    halved = n // 2
    half = prefix_ref.shape[0] // CORES // 2
    blocks, outs = refs[: len(refs) - n], refs[len(refs) - n :]
    prefixes = keys.shape[0]
    requests, _, spots = tails.shape
    slots = spots // CORES
    per = blocks[0].shape[1]
    wide_tiles = LAT // LANES
    total = n * per
    core = core_ref[0]

    for p in range(prefixes):
        counts[p] = 0

    def sort(r, carry):
        p = prefix_ref[core * requests + r]
        at = counts[p]
        members[p * requests + at] = r
        counts[p] = at + 1
        return carry

    lax.fori_loop(0, requests, sort, 0)

    def key_copy(p):
        return pltpu.make_async_copy(sorted_keys.at[p], keys.at[p], key_sems.at[p])

    def load(p, carry):
        key_copy(p).start()

        def tail(i, carry):
            r = members[p * requests + i]
            mine, theirs = tails.at[r, :, pl.ds(0, slots)], tails.at[r, :, pl.ds(slots, slots)]
            pltpu.make_async_copy(own_suffix.at[core * requests + r], mine, tail_sems.at[r]).start()
            pltpu.make_async_copy(other_suffix.at[core * requests + r], theirs, tail_sems.at[r]).start()
            return carry

        lax.fori_loop(0, counts[p], tail, 0)
        return carry

    lax.fori_loop(0, prefixes, load, 0)
    stats[...] = jnp.zeros_like(stats)
    nt = (((1,), (1,)), ((), ()))

    def fetch(r, base):
        for k in range(n):
            span = pl.ds(base + k * per, per)
            if k != halved:
                heads[span] = blocks[k][r]
                continue

            @pl.when(r < half)
            def _():
                heads[span] = blocks[k][r]

            @pl.when(r >= half)
            def _():
                heads[span] = blocks[n][r - half]

    def split(w):
        high = w.astype(jnp.bfloat16)
        low = (w - high.astype(jnp.float32)).astype(jnp.bfloat16)
        return jnp.concatenate([high, low], axis=0)

    def group(p, i):
        last = counts[p] - 1
        rs = [members[p * requests + jnp.minimum(WIDE * i + j, last)] for j in range(WIDE)]
        for j in range(WIDE):
            fetch(rs[j], j * total)

            @pl.when(WIDE * i + j <= last)
            def _():
                pltpu.make_async_copy(tails.at[rs[j]], tails.at[rs[j]], tail_sems.at[rs[j]]).wait()

        q = heads[...]
        cuts = keys.shape[1] // PARTS
        fronts, tops = [], []
        for c in range(PARTS):
            part = keys[p, c * cuts : (c + 1) * cuts]
            f = lax.dot_general(q, part, nt, preferred_element_type=jnp.float32)
            fronts.append(f)
            tops.append(jnp.max(f, axis=1, keepdims=True))
        slot = lax.broadcasted_iota(jnp.int32, (total, spots), 1)
        o, sums = None, None
        best = functools.reduce(jnp.maximum, tops)
        ends, edge = [], []
        for j in range(WIDE):
            s = jnp.dot(q[j * total : (j + 1) * total], tails[rs[j]], preferred_element_type=jnp.float32)
            mine, theirs = live_ref[rs[j]], live_ref[requests + rs[j]]
            limit = jnp.where(slot < slots, mine, theirs + slots)
            s = jnp.where(slot < limit, s, -jnp.inf)
            ends.append(s)
            edge.append(jnp.max(s, axis=1, keepdims=True))
        top = jnp.maximum(best, jnp.concatenate(edge, axis=0)).astype(jnp.bfloat16).astype(jnp.float32)
        for c in range(PARTS):
            w = jnp.exp2((fronts[c] - tops[c]) * LOG2_SCALE)
            fix = jnp.exp2((tops[c] - top) * LOG2_SCALE)
            t = jnp.dot(split(w), keys[p, c * cuts : (c + 1) * cuts, :LAT], preferred_element_type=jnp.float32)
            t = (t[: WIDE * total] + t[WIDE * total :]) * fix
            l = jnp.sum(w, axis=1, keepdims=True) * fix
            o, sums = (t, l) if o is None else (o + t, sums + l)
        for j in range(WIDE):
            r = rs[j]
            here = slice(j * total, (j + 1) * total)
            w = jnp.exp2((ends[j] - top[here]) * LOG2_SCALE)
            l = sums[here] + jnp.sum(w, axis=1, keepdims=True)
            t = lax.dot_general(split(w), tails[r, :LAT], nt, preferred_element_type=jnp.float32)
            res = o[here] + t[:total] + t[total:]
            for k in range(n):
                for t in range(wide_tiles):
                    tile = res[k * per : (k + 1) * per, t * LANES : (t + 1) * LANES]
                    span = pl.ds((r * wide_tiles + t) * per, per)
                    outs[k][span] = tile.astype(outs[k].dtype)
            lane = lax.broadcasted_iota(jnp.int32, stats.shape, 1)
            high = l.astype(jnp.bfloat16).astype(jnp.float32)
            new = jnp.where(lane == r, top[here], stats[...])
            new = jnp.where(lane == requests + r, high, new)
            stats[...] = jnp.where(lane == 2 * requests + r, l - high, new)

    def prefix(p, carry):
        key_copy(p).wait()
        lax.fori_loop(0, (counts[p] + WIDE - 1) // WIDE, lambda i, c: (group(p, i), c)[1], 0)
        return carry

    lax.fori_loop(0, prefixes, prefix, 0)

    for k in range(n):
        outs[k][pl.ds(requests * wide_tiles * per, per)] = stats[k * per : (k + 1) * per].astype(outs[k].dtype)


def merge_kernel(*refs):
    parts, out = refs[:-1], refs[-1]
    per, requests, _ = out.shape
    tiles = LAT // LANES
    stats = [p[requests * tiles * per : (requests * tiles + 1) * per].astype(jnp.float32) for p in parts]
    tops = [s[:, :requests] for s in stats]
    sums = [s[:, requests : 2 * requests] + s[:, 2 * requests : 3 * requests] for s in stats]
    top = functools.reduce(jnp.maximum, tops)
    scales = [jnp.exp2((t - top) * LOG2_SCALE) for t in tops]
    l = functools.reduce(jnp.add, [s * f for s, f in zip(sums, scales)])
    lane = lax.broadcasted_iota(jnp.int32, (per, LANES), 1)
    for r in range(requests):
        columns = [f[:, r : r + 1] for f in scales]
        for t in range(tiles):
            acc = None
            for part, f in zip(parts, columns):
                first = (r * tiles + t) * per
                term = part[first : first + per].astype(jnp.float32) * f
                acc = term if acc is None else acc + term
            out[:, r, t * LANES : (t + 1) * LANES] = acc
        out[:, r, LAT:] = jnp.where(lane == 0, top[:, r : r + 1], l[:, r : r + 1])


def finish_kernel(parts, out):
    peers = parts.shape[0]
    for h in range(parts.shape[1]):
        tops = [parts[j, h, :, LAT : LAT + 1] for j in range(peers)]
        top = functools.reduce(jnp.maximum, tops)
        acc, l = None, None
        for j in range(peers):
            f = jnp.exp2((tops[j] - top) * LOG2_SCALE)
            a = parts[j, h, :, :LAT] * f
            b = parts[j, h, :, LAT + 1 : LAT + 2] * f
            acc, l = (a, b) if acc is None else (acc + a, l + b)
        out[h] = (acc / l).astype(out.dtype)


def stage(core, labels, own_pool, other_pool, prefixes):
    held, rows, channels = own_pool.shape
    keys = (prefixes, CORES * held // prefixes * rows, channels)
    own_pool = pltpu.with_memory_space_constraint(own_pool, pltpu.HBM)
    return pl.pallas_call(
        stage_kernel,
        out_shape=pltpu.HBM(keys, jnp.bfloat16),
        in_specs=[SMEM] * 2 + [ANY] * 2,
        out_specs=ANY,
        scratch_shapes=[
            pltpu.VMEM(keys, jnp.bfloat16),
            pltpu.SMEM((prefixes,), jnp.int32),
            pltpu.SemaphoreType.DMA((2 * prefixes,)),
        ],
        compiler_params=pltpu.CompilerParams(vmem_limit_bytes=8 * 2**20),
        cost_estimate=pl.CostEstimate(flops=4 * 10**9, bytes_accessed=0, transcendentals=0),
        name="stage",
    )(core, labels, own_pool, other_pool)


def attend(core, prefix_of, live, keys, own_suffix, other_suffix, blocks, dtypes):
    n = len(dtypes)
    half, per, channels = blocks[0].shape
    prefixes = keys.shape[0]
    tails = (half, channels, CORES * other_suffix.shape[2])
    flops = 6 * half * n * per * channels * (keys.shape[1] + tails[2])
    keys, own_suffix, other_suffix = (
        pltpu.with_memory_space_constraint(a, pltpu.HBM) for a in (keys, own_suffix, other_suffix)
    )
    return pl.pallas_call(
        attend_kernel,
        out_shape=[jax.ShapeDtypeStruct(((half * (LAT // LANES) + 1) * per, LANES), t) for t in dtypes],
        in_specs=[SMEM] * 3 + [ANY] * 3 + [VMEM] * len(blocks),
        out_specs=[VMEM] * n,
        scratch_shapes=[
            pltpu.VMEM(keys.shape, jnp.bfloat16),
            pltpu.VMEM(tails, jnp.bfloat16),
            pltpu.VMEM((n * per, LANES), jnp.float32),
            pltpu.VMEM((WIDE * n * per, channels), jnp.bfloat16),
            pltpu.SMEM((prefixes * half,), jnp.int32),
            pltpu.SMEM((prefixes,), jnp.int32),
            pltpu.SemaphoreType.DMA((prefixes,)),
            pltpu.SemaphoreType.DMA((half,)),
        ],
        compiler_params=pltpu.CompilerParams(vmem_limit_bytes=36 * 2**20),
        cost_estimate=pl.CostEstimate(flops=flops, bytes_accessed=0, transcendentals=0),
        name="attend",
    )(core, prefix_of, live, keys, own_suffix, other_suffix, *blocks)


def body(torus, queries, prefix_pool, block_table, prefix_of, suffix_cache, suffix_len):
    side = torus.side
    held, _, channels = prefix_pool.shape
    prefixes = block_table.shape[0]
    reqs, slots, _ = suffix_cache.shape
    half = reqs // CORES
    position = lax.axis_index("seq")
    core = position % CORES

    q = queries.reshape(CORES, half, channels)
    mine, theirs = q[core], q[1 - core]
    theirs = torus.partner(theirs)
    suffix = jnp.swapaxes(suffix_cache, 1, 2)
    pool, theirs = lax.optimization_barrier((prefix_pool, theirs))
    pair_q = jnp.stack([mine, theirs])
    other_pool = torus.partner(pool)
    other_suffix = torus.partner(suffix)

    first_block = (position - core) * held
    ids = first_block + lax.iota(jnp.int32, CORES * held)
    named = jnp.any(block_table[:, :, None] == ids[None, None, :], axis=1)
    labels = jnp.sum(named.astype(jnp.int32) * lax.iota(jnp.int32, prefixes)[:, None], axis=0)
    lengths = lax.dynamic_slice_in_dim(suffix_len, core * half, half, 0)
    live = jnp.concatenate([lengths - position * slots, lengths - (position ^ 1) * slots])

    spread = jnp.broadcast_to(pair_q[None], (side,) + pair_q.shape)
    line = lax.all_to_all(spread, "seq", 0, 0, axis_index_groups=torus.groups(True))
    per = side * CORES
    block = jnp.swapaxes(line.reshape(per, half, channels), 0, 1)

    order = (4, 3, side - 3, 2, side - 2, 1, side - 1)
    got = {0: block}
    mid = half // 2
    for k in (2, side - 2, 1, side - 1):
        got[k] = torus.shift(block, k)
    got[4] = torus.shift(got[2][:mid], 2)
    got[side] = torus.shift(got[side - 2][mid:], side - 2)
    got[3] = torus.shift(got[2], 1)
    got[side - 3] = torus.shift(got[side - 2], side - 1)

    core = core.reshape(1)
    keys = stage(core, labels, prefix_pool, other_pool, prefixes)
    types = [jnp.float32] + [jnp.bfloat16] * (side - 1)
    outs = attend(core, prefix_of, live, keys, suffix, other_suffix, [got[k] for k in range(side + 1)], types)
    parts = [outs[0]] + [torus.shift(outs[k], side - k) for k in order]
    merged = pl.pallas_call(
        merge_kernel,
        out_shape=jax.ShapeDtypeStruct((per, half, LAT + 128), jnp.float32),
        in_specs=[VMEM] * side,
        out_specs=VMEM,
        compiler_params=pltpu.CompilerParams(vmem_limit_bytes=16 * 2**20),
        name="merge",
    )(*parts)
    shares = lax.all_to_all(
        merged.reshape(side, CORES, half, LAT + 128), "seq", 0, 0, axis_index_groups=torus.groups(True)
    )
    context = pl.pallas_call(
        finish_kernel,
        out_shape=jax.ShapeDtypeStruct((CORES, half, LAT), jnp.bfloat16),
        in_specs=[VMEM],
        out_specs=VMEM,
        compiler_params=pltpu.CompilerParams(vmem_limit_bytes=8 * 2**20),
        name="finish",
    )(shares)
    back = torus.partner(context[1])
    both = jnp.where(core[0] == 0, jnp.stack([context[0], back]), jnp.stack([back, context[0]]))
    return both.reshape(reqs, 1, LAT)


def solution(mesh):
    torus = Torus(mesh.shape["seq"])

    def step(*args):
        return body(torus, *args)

    return jax.shard_map(
        step,
        mesh=mesh,
        in_specs=(
            P("groups", "seq", None),
            P(("groups", "seq"), None, None),
            P("groups", None),
            P("groups"),
            P("groups", "seq", None),
            P("groups"),
        ),
        out_specs=P("groups", "seq", None),
        check_vma=False,
    )
```
